256 devices in a mesh: gz: 8 (over z_hi, y), xy: 32 (over z_lo, x, core).
Axes of the slice: x: 4, y: 4, z: 8 (z_hi: 2, z_lo: 4; z = z_hi * 4 + z_lo), core: 2. Of those that a mesh axis runs over, the one named last changes fastest.
Arguments:
- stack: bfloat16 [128, 512, 2048], P('gz', 'xy'), may hold values from -8 to 8
Outputs:
- joined: float32 [512, 2048], P('xy', 'gz')
- pooled: float32 [256, 1024], P('xy', 'gz')
The draws below stay inside these ranges and needn't reach their ends.
All inputs are finite; a program needn't handle non-finite values.
Results may differ from the reference program's by a relative error of at most 0.0003.
Values may be sent and summed in bfloat16 or wider, within the bound.
No kernel may reach another device: no remote copies, remote signals or barrier semaphores. Data moves between devices by JAX's collectives and lax.ppermute only.
A program may use at most 128 MiB of HBM per device.

```python
import jax
import jax.numpy as jnp
from jax import lax

PLANES = 128
HEIGHT = 512
WIDTH = 2048


def draw_stack(key, part):
    key_amp, key_base = jax.random.split(key, 2)
    amp_log = jax.random.uniform(key_amp, (PLANES, HEIGHT // 8, WIDTH // 8), jnp.float32, jnp.log(0.04), jnp.log(0.4))
    amplitude = jnp.repeat(jnp.repeat(jnp.exp(amp_log), 8, axis=1), 8, axis=2)
    texture = jax.random.normal(key_base, (PLANES, HEIGHT, WIDTH), jnp.float32)
    stack = jnp.clip(texture * amplitude, -8.0, 8.0)
    return stack.astype(jnp.bfloat16)


def setup_inputs(seed: int = 0) -> dict:
    key_of = jax.random.split(jax.random.key(seed), 2)
    return {
        "stack": draw_stack(jax.random.fold_in(key_of[1], 71), 0),
    }


sharpness = 0.016
laplace_taps = ((0, 0, 16.0), (1, 0, -2.0), (-1, 0, -2.0), (0, 1, -2.0), (0, -1, -2.0), (1, 1, -1.0), (1, -1, -1.0), (-1, 1, -1.0), (-1, -1, -1.0), (2, 0, -1.0), (-2, 0, -1.0), (0, 2, -1.0), (0, -2, -1.0))


def plane_score(plane):
    height, breadth = plane.shape
    padded = jnp.pad(plane.astype(jnp.float32), 2)
    laplace_out = jnp.zeros((height, breadth), jnp.float32)
    for row_step, col_step, weight in laplace_taps:
        laplace_out = laplace_out + weight * padded[2 + row_step:2 + row_step + height, 2 + col_step:2 + col_step + breadth]
    energy = laplace_out * laplace_out
    padded_energy = jnp.pad(energy, 2)
    row_total = jnp.zeros((height, breadth + 4), jnp.float32)
    for shift_amount in range(-2, 3):
        row_total = row_total + padded_energy[2 + shift_amount:2 + shift_amount + height, :]
    box_total = jnp.zeros((height, breadth), jnp.float32)
    for shift_amount in range(-2, 3):
        box_total = box_total + row_total[:, 2 + shift_amount:2 + shift_amount + breadth]
    return box_total * sharpness


def reference(stack):
    height, breadth = stack.shape[1], stack.shape[2]

    def advance(carry, plane):
        running_max, weighted_sum, weight_sum = carry
        score = plane_score(plane)
        new_max = jnp.maximum(running_max, score)
        old_scale = jnp.exp(running_max - new_max)
        new_scale = jnp.exp(score - new_max)
        weighted_sum = weighted_sum * old_scale + new_scale * plane.astype(jnp.float32)
        weight_sum = weight_sum * old_scale + new_scale
        return (new_max, weighted_sum, weight_sum), None

    start = (jnp.full((height, breadth), -1e30, jnp.float32), jnp.zeros((height, breadth), jnp.float32), jnp.zeros((height, breadth), jnp.float32))
    (final_max, weighted_sum, weight_sum), unused = lax.scan(advance, start, stack)
    joined = weighted_sum / weight_sum
    pooled = joined.reshape(height // 2, 2, breadth // 2, 2).mean(axis=(1, 3))
    return joined, pooled
```

```python
import functools

import jax
import jax.numpy as jnp
from jax import lax
from jax.experimental import pallas as pl
from jax.experimental.pallas import tpu as pltpu
from jax.sharding import PartitionSpec as P

sharpness = 0.016
log2e = 1.4426950408889634
LANES = 128
HALO = 4


def shifted(tiles, step, lane, before=None):
    turned = [pltpu.roll(t, (-step) % LANES, axis=1) for t in tiles]
    blank = jnp.zeros_like(tiles[0])
    out = []
    for j in range(len(tiles)):
        if step > 0:
            other = turned[j + 1] if j + 1 < len(tiles) else blank
            out.append(jnp.where(lane < LANES - step, turned[j], other))
        else:
            other = turned[j - 1] if j > 0 else (blank if before is None else before)
            out.append(jnp.where(lane >= -step, turned[j], other))
    return out


def energy_row(load, count, lane):
    mids, cores, bases = [], [], []
    for j in range(count):
        core = load(2, j)
        near = load(1, j) + load(3, j)
        far = load(0, j) + load(4, j)
        mid = (core + core) + near
        mids.append(mid)
        cores.append(core)
        bases.append(20.0 * core - (mid + mid) - far)
    up1, down1 = shifted(mids, 1, lane), shifted(mids, -1, lane)
    up2, down2 = shifted(cores, 2, lane), shifted(cores, -2, lane)
    out = []
    for j in range(count):
        lap = bases[j] - (up1[j] + down1[j]) - (up2[j] + down2[j])
        out.append(lap * lap)
    return out


def partials_row(energy, cells, count, lane):
    cols = []
    for j in range(count):
        cols.append(((energy(0, j) + energy(1, j)) + (energy(3, j) + energy(4, j))) + energy(2, j))
    pairs = [a + b for a, b in zip(cols, shifted(cols, 1, lane))]
    before = jnp.where(lane == 1, pltpu.roll(cols[0], 1, axis=1), 0.0)
    fours = [a + b for a, b in zip(pairs, shifted(pairs, -2, lane, before))]
    fives = [a + b for a, b in zip(fours, shifted(cols, 2, lane))]
    out = []
    for j in range(count):
        score = fives[j] * (sharpness * log2e)
        top = jnp.max(score, axis=0, keepdims=True)
        weight = jnp.exp2(score - top)
        total = jnp.sum(weight, axis=0, keepdims=True)
        blend = jnp.sum(weight * cells(j), axis=0, keepdims=True)
        out.append((top, total, blend))
    return out


def tile(j):
    return pl.ds(j * LANES, LANES)


def turn_kernel(x_ref, xt_ref, a_ref, b_ref, swap, *, chunk):
    planes, rows, cols = x_ref.shape
    n = planes * rows
    o = lax.broadcasted_iota(jnp.int32, (n, n), 0)
    i = lax.broadcasted_iota(jnp.int32, (n, n), 1)
    hit = (o // planes == i % rows) & (o % planes == i // rows)
    swap[...] = jnp.where(hit, 1.0, 0.0).astype(jnp.bfloat16)
    odd = lax.rem(lax.axis_index("xy"), 2)
    last = rows - HALO
    for c in range(cols // chunk):
        ds = pl.ds(c * chunk, chunk)
        x = x_ref[:, :, ds].reshape(n, chunk)
        y = jnp.dot(swap[...], x, preferred_element_type=jnp.float32)
        xt_ref[:, :, ds] = y.reshape(rows, planes, chunk)
    a_ref[...] = xt_ref[pl.ds(last - odd * last, HALO)].astype(jnp.bfloat16)
    b_ref[...] = xt_ref[pl.ds(odd * last, HALO)].astype(jnp.bfloat16)


def inner_kernel(xt_ref, edge_ref, part_ref, energy):
    rows, planes, cols = xt_ref.shape
    count = cols // LANES
    lane = lax.broadcasted_iota(jnp.int32, (planes, LANES), 1)

    def first(r, carry):
        row = energy_row(lambda k, j: xt_ref[r + k, :, tile(j)], count, lane)
        for j in range(count):
            energy[r, :, tile(j)] = row[j]
        return carry

    lax.fori_loop(0, rows - 4, first, 0)
    edge_ref[0:4] = energy[0:4]
    edge_ref[4:8] = energy[rows - 8:rows - 4]

    for r in range(rows - 8):
        row = partials_row(
            lambda k, j: energy[r + k, :, tile(j)], lambda j: xt_ref[r + 4, :, tile(j)], count, lane
        )
        for j in range(count):
            for q in range(3):
                part_ref[q, pl.ds(r, 1), tile(j)] = row[j][q]


def outer_kernel(xt_ref, a_ref, b_ref, edge_ref, inner_ref, out_ref, cells, energy, part):
    rows, planes, cols = xt_ref.shape
    count = cols // LANES
    lane = lax.broadcasted_iota(jnp.int32, (planes, LANES), 1)
    me = lax.axis_index("xy")
    odd = lax.rem(me, 2)
    cells[pl.ds(12 - 12 * odd, 4)] = a_ref[...].astype(jnp.float32)
    cells[pl.ds(12 * odd, 4)] = b_ref[...].astype(jnp.float32)
    cells[4:8] = xt_ref[0:4]
    cells[8:12] = xt_ref[rows - 4:rows]
    energy[4:8] = edge_ref[0:4]
    energy[8:12] = edge_ref[4:8]
    above = jnp.where(me > 0, 1.0, 0.0)
    below = jnp.where(me < lax.axis_size("xy") - 1, 1.0, 0.0)

    def first(i, carry):
        side, k0 = i // 4, lax.rem(i, 4)
        row = energy_row(lambda k, j: cells[8 * side + k0 + k, :, tile(j)], count, lane)
        outside = jnp.where(side == 0, jnp.where(k0 < 2, 1 - above, 0.0), jnp.where(k0 >= 2, 1 - below, 0.0))
        keep = 1.0 - outside
        for j in range(count):
            energy[12 * side + k0, :, tile(j)] = row[j] * keep
        return carry

    lax.fori_loop(0, 8, first, 0)
    part[:, 4:rows - 4, :] = inner_ref[...]

    for i in range(8):
        side, k0 = i // 4, i % 4
        base = 8 * side + k0
        row = partials_row(
            lambda k, j: energy[base + k, :, tile(j)], lambda j: cells[4 + 4 * side + k0, :, tile(j)], count, lane
        )
        for j in range(count):
            for q in range(3):
                part[q, pl.ds((rows - 4) * side + k0, 1), tile(j)] = row[j][q]
    groups, _, own = out_ref.shape
    for g in range(groups):
        ds = pl.ds(g * own, own)
        total = part[1, :, ds]
        out_ref[g, 0:rows, :] = part[0, :, ds] + jnp.log2(total)
        out_ref[g, rows:2 * rows, :] = part[2, :, ds] / total


def join_kernel(in_ref, joined_ref, pooled_ref):
    groups, twice, own = in_ref.shape
    rows = twice // 2
    logs = [in_ref[g, 0:rows, :] for g in range(groups)]
    top = functools.reduce(jnp.maximum, logs)
    weights = [jnp.exp2(v - top) for v in logs]
    total = functools.reduce(jnp.add, weights)
    blend = functools.reduce(jnp.add, [w * in_ref[g, rows:twice, :] for g, w in enumerate(weights)])
    joined = blend / total
    joined_ref[...] = joined
    r = lax.broadcasted_iota(jnp.int32, (rows // 2, rows), 0)
    c = lax.broadcasted_iota(jnp.int32, (rows // 2, rows), 1)
    row_pairs = jnp.where(c // 2 == r, 0.25, 0.0)
    r = lax.broadcasted_iota(jnp.int32, (own, own // 2), 0)
    c = lax.broadcasted_iota(jnp.int32, (own, own // 2), 1)
    col_pairs = jnp.where(r // 2 == c, 1.0, 0.0)
    exact = lax.Precision.HIGHEST
    halves = jnp.dot(row_pairs, joined, preferred_element_type=jnp.float32, precision=exact)
    pooled_ref[...] = jnp.dot(halves, col_pairs, preferred_element_type=jnp.float32, precision=exact)


def vmem(count):
    return [pl.BlockSpec(memory_space=pltpu.VMEM)] * count


def params(mib):
    return pltpu.CompilerParams(vmem_limit_bytes=mib << 20)


def shards(stack):
    planes, rows, cols = stack.shape
    f32, bf16 = jnp.float32, jnp.bfloat16
    sds = jax.ShapeDtypeStruct
    strip = sds((HALO, planes, cols), bf16)
    xt, to_a, to_b = pl.pallas_call(
        functools.partial(turn_kernel, chunk=512),
        out_shape=(sds((rows, planes, cols), f32), strip, strip),
        in_specs=vmem(1),
        out_specs=tuple(vmem(3)),
        scratch_shapes=[pltpu.VMEM((planes * rows, planes * rows), bf16)],
        compiler_params=params(8),
        cost_estimate=pl.CostEstimate(flops=10**7, bytes_accessed=4 << 20, transcendentals=0),
        name="turn",
    )(stack)
    count = lax.axis_size("xy")
    ends = [(i, i + 1) for i in range(1, count - 1, 2)]
    from_b = lax.ppermute(to_b, "xy", ends + [(j, i) for i, j in ends])
    from_a = lax.ppermute(to_a, "xy", [(i, i ^ 1) for i in range(count)])
    edge, inner = pl.pallas_call(
        inner_kernel,
        out_shape=(sds((8, planes, cols), f32), sds((3, rows - 8, cols), f32)),
        in_specs=vmem(1),
        out_specs=tuple(vmem(2)),
        scratch_shapes=[pltpu.VMEM((rows - 4, planes, cols), f32)],
        compiler_params=params(16),
        cost_estimate=pl.CostEstimate(flops=10**8, bytes_accessed=4 << 20, transcendentals=10**6),
        name="inner",
    )(xt)
    groups = lax.axis_size("gz")
    own = cols // groups
    ready = pl.pallas_call(
        outer_kernel,
        out_shape=sds((groups, 2 * rows, own), f32),
        in_specs=vmem(5),
        out_specs=vmem(1)[0],
        scratch_shapes=[
            pltpu.VMEM((16, planes, cols), f32),
            pltpu.VMEM((16, planes, cols), f32),
            pltpu.VMEM((3, rows, cols), f32),
        ],
        compiler_params=params(16),
        cost_estimate=pl.CostEstimate(flops=10**8, bytes_accessed=4 << 20, transcendentals=10**6),
        name="outer",
    )(xt, from_a, from_b, edge, inner)
    parts = lax.all_to_all(ready, "gz", split_axis=0, concat_axis=0, tiled=True)
    return pl.pallas_call(
        join_kernel,
        out_shape=(sds((rows, own), f32), sds((rows // 2, own // 2), f32)),
        in_specs=vmem(1),
        out_specs=tuple(vmem(2)),
        compiler_params=params(4),
        name="join",
    )(parts)


def solution(mesh):
    in_specs = (P("gz", "xy", None),)
    out_specs = (P("xy", "gz"), P("xy", "gz"))
    return jax.shard_map(shards, mesh=mesh, in_specs=in_specs, out_specs=out_specs, check_vma=False)
```

```python
import functools

import jax
import jax.numpy as jnp
from jax import lax
from jax.experimental import pallas as pl
from jax.experimental.pallas import tpu as pltpu
from jax.sharding import PartitionSpec as P


sharpness = 0.016
log2e = 1.4426950408889634
LANES = 128
HALO = 4
UNROLL = 2


def tile(j):
    return pl.ds(j * LANES, LANES)


def moved(turned, j, step, lane):
    if step > 0:
        other = turned[j + 1] if j + 1 < len(turned) else jnp.zeros_like(turned[j])
        return jnp.where(lane < LANES - step, turned[j], other)
    other = turned[j - 1] if j > 0 else jnp.zeros_like(turned[j])
    return jnp.where(lane >= -step, turned[j], other)


def rotated(tiles, step):
    return [pltpu.roll(t, (-step) % LANES, axis=1) for t in tiles]


def energy_row(load, count, lane):
    cells = [load(2, j) for j in range(count)]
    besides = [(c + c) + (load(1, j) + load(3, j)) for j, c in enumerate(cells)]
    up1, down1 = rotated(besides, 1), rotated(besides, -1)
    up2, down2 = rotated(cells, 2), rotated(cells, -2)
    for j in range(count):
        middle = (20.0 * cells[j] - (besides[j] + besides[j])) - (load(0, j) + load(4, j))
        lap = (
            middle
            - (moved(up1, j, 1, lane) + moved(down1, j, -1, lane))
            - (moved(up2, j, 2, lane) + moved(down2, j, -2, lane))
        )
        yield j, lap * lap


def gather_sum(tiles, sub):
    low = sub < 4
    tiles = [
        jnp.where(low, a, b) + pltpu.roll(jnp.where(low, b, a), 4, axis=0) for a, b in zip(tiles[:4], tiles[4:])
    ]
    for d in (2, 1):
        pick = (sub & d) == 0
        tiles = [
            jnp.where(pick, a + pltpu.roll(a, 8 - d, axis=0), b + pltpu.roll(b, d, axis=0))
            for a, b in zip(tiles[:d], tiles[d:])
        ]
    return tiles[0]


def partials_row(energy, cell, store, count, lane, sub):
    cols = [((energy(0, j) + energy(1, j)) + (energy(3, j) + energy(4, j))) + energy(2, j) for j in range(count)]
    turned = {step: rotated(cols, step) for step in (1, -1, 2, -2)}
    for block in range(0, count, 8):
        tops, totals, blends = None, [], []
        for j in range(block, block + 8):
            box = cols[j] + ((moved(turned[1], j, 1, lane) + moved(turned[-1], j, -1, lane)) + (
                moved(turned[2], j, 2, lane) + moved(turned[-2], j, -2, lane)))
            score = box * (sharpness * log2e)
            top = jnp.max(score, axis=0, keepdims=True)
            weight = jnp.exp2(score - top)
            blend = weight * cell(j)
            totals.append(weight[0:8] + weight[8:16])
            blends.append(blend[0:8] + blend[8:16])
            tall = jnp.broadcast_to(top, (8, LANES))
            tops = tall if tops is None else jnp.where(sub == j - block, tall, tops)
        total = gather_sum(totals, sub)
        store(0, block, tops + jnp.log2(total))
        store(1, block, gather_sum(blends, sub) / total)


def grid_of(rows, cols):
    return lax.broadcasted_iota(jnp.int32, (rows, cols), 0), lax.broadcasted_iota(jnp.int32, (rows, cols), 1)


def lanes_and_subs(planes):
    return (
        lax.broadcasted_iota(jnp.int32, (planes, LANES), 1),
        lax.broadcasted_iota(jnp.int32, (8, LANES), 0),
    )


def turn_kernel(x_ref, xt_ref, a_ref, b_ref, *, chunk):
    planes, rows, cols = x_ref.shape
    n = planes * rows
    o, k = grid_of(n, n)
    swap = jnp.where((o // planes == k % rows) & (o % planes == k // rows), 1.0, 0.0).astype(jnp.bfloat16)
    for c in range(cols // chunk):
        ds = pl.ds(c * chunk, chunk)
        y = jnp.dot(swap, x_ref[:, :, ds].reshape(n, chunk), preferred_element_type=jnp.float32)
        xt_ref[:, :, ds] = y.reshape(rows, planes, chunk)
    odd = lax.rem(lax.axis_index("xy"), 2)
    last = rows - HALO
    a_ref[...] = xt_ref[pl.ds(last - odd * last, HALO)].astype(jnp.bfloat16)
    b_ref[...] = xt_ref[pl.ds(odd * last, HALO)].astype(jnp.bfloat16)


def inner_kernel(xt_ref, energy_ref, part_ref):
    rows, planes, cols = xt_ref.shape
    count = cols // LANES
    lane, sub = lanes_and_subs(planes)

    def first(r, carry):
        for j, value in energy_row(lambda k, j: xt_ref[r + k, :, tile(j)], count, lane):
            energy_ref[r, :, tile(j)] = value
        return carry

    lax.fori_loop(0, rows - 4, first, 0, unroll=UNROLL)

    def second(r, carry):
        def store(q, block, value):
            part_ref[q, r, block:block + 8, :] = value

        partials_row(
            lambda k, j: energy_ref[r + k, :, tile(j)], lambda j: xt_ref[r + 4, :, tile(j)], store, count, lane, sub
        )
        return carry

    lax.fori_loop(0, rows - 8, second, 0, unroll=UNROLL)


def side_rows(below, xt_ref, got_ref, energy_ref, part, cells, energy):
    rows, planes, cols = xt_ref.shape
    count = cols // LANES
    lane, sub = lanes_and_subs(planes)
    me = lax.axis_index("xy")
    at_end = me == jnp.where(below == 1, lax.axis_size("xy") - 1, 0)
    flip = 3 * below
    for i in range(HALO):
        cells[i] = got_ref[i ^ flip].astype(jnp.float32)
        cells[HALO + i] = xt_ref[(rows - HALO) * below + (i ^ flip)]
        energy[HALO + i] = energy_ref[(rows - 8) * below + (i ^ flip)]

    def first(i, carry):
        keep = jnp.where((i < 2) & at_end, 0.0, 1.0)
        for j, value in energy_row(lambda k, j: cells[i + k, :, tile(j)], count, lane):
            energy[i, :, tile(j)] = value * keep
        return carry

    lax.fori_loop(0, HALO, first, 0, unroll=UNROLL)

    def second(i, carry):
        def store(q, block, value):
            part[q, HALO * below + (i ^ flip), block:block + 8, :] = value

        partials_row(
            lambda k, j: energy[i + k, :, tile(j)], lambda j: cells[HALO + i, :, tile(j)], store, count, lane, sub
        )
        return carry

    lax.fori_loop(0, HALO, second, 0, unroll=UNROLL)


def near_kernel(xt_ref, got_ref, energy_ref, part_ref, cells, energy):
    below = 1 - lax.rem(lax.axis_index("xy"), 2)
    side_rows(below, xt_ref, got_ref, energy_ref, part_ref, cells, energy)


def far_kernel(xt_ref, got_ref, energy_ref, inner_ref, near_ref, out_ref, cells, energy, part):
    rows, _, cols = xt_ref.shape
    count = cols // LANES
    below = lax.rem(lax.axis_index("xy"), 2)
    side_rows(below, xt_ref, got_ref, energy_ref, part, cells, energy)
    for q in range(2):
        for i in range(HALO):
            slot = HALO * (1 - below) + i
            part[q, slot] = near_ref[q, slot]
    each = count // out_ref.shape[0]
    for q in range(2):
        for h, ref in enumerate((inner_ref, part)):
            for j in range(count):
                flat = ref.at[q].reshape(8 * count, LANES)
                out_ref[j // each, q * rows + 8 * h:q * rows + 8 * h + 8, tile(j % each)] = (
                    flat[pl.ds(j, 8, stride=count), :]
                )


def join_kernel(in_ref, joined_ref, pooled_ref, half):
    groups, twice, own = in_ref.shape
    rows = twice // 2
    logs = [in_ref[g, 0:rows, :] for g in range(groups)]
    top = functools.reduce(jnp.maximum, logs)
    weights = [jnp.exp2(v - top) for v in logs]
    total = functools.reduce(jnp.add, weights)
    blend = functools.reduce(jnp.add, [w * in_ref[g, rows:twice, :] for g, w in enumerate(weights)])
    joined = blend / total
    joined_ref[HALO:HALO + 8, :] = joined[0:8]
    joined_ref[0:HALO, :] = joined[8:12]
    joined_ref[HALO + 8:rows, :] = joined[12:16]
    halves = []
    for h in range(own // LANES):
        half[h] = joined_ref[:, tile(h)]
        even, uneven = (half.at[h][pl.ds(k, rows // 2, stride=2), :] for k in range(2))
        halves.append(even + uneven)
    halves = jnp.concatenate(halves, axis=1)
    r, c = grid_of(own, own // 2)
    col_pairs = jnp.where(r // 2 == c, 0.25, 0.0)
    pooled_ref[...] = jnp.dot(
        halves, col_pairs, preferred_element_type=jnp.float32, precision=lax.Precision.HIGHEST
    )


def vmem(count):
    return [pl.BlockSpec(memory_space=pltpu.VMEM)] * count


def params(mib):
    return pltpu.CompilerParams(vmem_limit_bytes=mib << 20)


def cost(flops):
    return pl.CostEstimate(flops=flops, bytes_accessed=4 << 20, transcendentals=10**6)


def shards(stack):
    planes, rows, cols = stack.shape
    f32, bf16 = jnp.float32, jnp.bfloat16
    sds = jax.ShapeDtypeStruct
    strip = sds((HALO, planes, cols), bf16)
    count = cols // LANES
    xt, to_a, to_b = pl.pallas_call(
        functools.partial(turn_kernel, chunk=512),
        out_shape=(sds((rows, planes, cols), f32), strip, strip),
        in_specs=vmem(1),
        out_specs=tuple(vmem(3)),
        compiler_params=params(8),
        cost_estimate=cost(10**7),
        name="turn",
    )(stack)
    devices = lax.axis_size("xy")
    ends = [(i, i + 1) for i in range(1, devices - 1, 2)]
    from_b = lax.ppermute(to_b, "xy", ends + [(j, i) for i, j in ends])
    from_a = lax.ppermute(to_a, "xy", [(i, i ^ 1) for i in range(devices)])
    energy, inner = pl.pallas_call(
        inner_kernel,
        out_shape=(sds((rows - 4, planes, cols), f32), sds((2, rows - 8, count, LANES), f32)),
        in_specs=vmem(1),
        out_specs=tuple(vmem(2)),
        compiler_params=params(8),
        cost_estimate=cost(10**8),
        name="inner",
    )(xt)
    side_scratch = [pltpu.VMEM((2 * HALO, planes, cols), f32)] * 2
    part = sds((2, 2 * HALO, count, LANES), f32)
    near = pl.pallas_call(
        near_kernel,
        out_shape=part,
        in_specs=vmem(3),
        out_specs=vmem(1)[0],
        scratch_shapes=side_scratch,
        compiler_params=params(8),
        cost_estimate=cost(10**8),
        name="near",
    )(xt, from_a, energy)
    groups = lax.axis_size("gz")
    own = cols // groups
    ready = pl.pallas_call(
        far_kernel,
        out_shape=sds((groups, 2 * rows, own), f32),
        in_specs=vmem(5),
        out_specs=vmem(1)[0],
        scratch_shapes=side_scratch + [pltpu.VMEM(part.shape, f32)],
        compiler_params=params(8),
        cost_estimate=cost(10**8),
        name="far",
    )(xt, from_b, energy, inner, near)
    parts = lax.all_to_all(ready, "gz", split_axis=0, concat_axis=0, tiled=True)
    return pl.pallas_call(
        join_kernel,
        out_shape=(sds((rows, own), f32), sds((rows // 2, own // 2), f32)),
        in_specs=vmem(1),
        out_specs=tuple(vmem(2)),
        scratch_shapes=[pltpu.VMEM((own // LANES, rows, LANES), f32)],
        compiler_params=params(4),
        name="join",
    )(parts)


def solution(mesh):
    in_specs = (P("gz", "xy", None),)
    out_specs = (P("xy", "gz"), P("xy", "gz"))
    return jax.shard_map(shards, mesh=mesh, in_specs=in_specs, out_specs=out_specs, check_vma=False)
```

```python
import functools

import jax
import jax.numpy as jnp
from jax import lax
from jax.experimental import pallas as pl
from jax.experimental.pallas import tpu as pltpu
from jax.sharding import PartitionSpec as P


sharpness = 0.016
log2e = 1.4426950408889634
LANES = 128
HALO = 4
UNROLL = 2
UNROLL2 = 1


def tile(j):
    return pl.ds(j * LANES, LANES)


def moved(turned, j, step, lane):
    if step > 0:
        other = turned[j + 1] if j + 1 < len(turned) else jnp.zeros_like(turned[j])
        return jnp.where(lane < LANES - step, turned[j], other)
    other = turned[j - 1] if j > 0 else jnp.zeros_like(turned[j])
    return jnp.where(lane >= -step, turned[j], other)


def rotated(tiles, step):
    return [pltpu.roll(t, (-step) % LANES, axis=1) for t in tiles]


def energy_row(load, count, lane):
    cells = [load(2, j) for j in range(count)]
    besides = [(c + c) + (load(1, j) + load(3, j)) for j, c in enumerate(cells)]
    up1, down1 = rotated(besides, 1), rotated(besides, -1)
    up2, down2 = rotated(cells, 2), rotated(cells, -2)
    for j in range(count):
        middle = (20.0 * cells[j] - (besides[j] + besides[j])) - (load(0, j) + load(4, j))
        lap = (
            middle
            - (moved(up1, j, 1, lane) + moved(down1, j, -1, lane))
            - (moved(up2, j, 2, lane) + moved(down2, j, -2, lane))
        )
        yield j, lap * lap


def gather_sum(tiles, sub):
    low = sub < 4
    tiles = [
        jnp.where(low, a, b) + pltpu.roll(jnp.where(low, b, a), 4, axis=0) for a, b in zip(tiles[:4], tiles[4:])
    ]
    for d in (2, 1):
        pick = (sub & d) == 0
        tiles = [
            jnp.where(pick, a + pltpu.roll(a, 8 - d, axis=0), b + pltpu.roll(b, d, axis=0))
            for a, b in zip(tiles[:d], tiles[d:])
        ]
    return tiles[0]


def box_of(cols, lane):
    count = len(cols)
    left = rotated(cols, -1)
    pairs = [c + moved(left, j, -1, lane) for j, c in enumerate(cols)]
    right = rotated(pairs, 2)
    after = jnp.where(lane == LANES - 2, pltpu.roll(cols[-1], LANES - 1, axis=1), 0.0)
    far = rotated(cols, -2)
    for j in range(count):
        other = right[j + 1] if j + 1 < count else after
        fours = pairs[j] + jnp.where(lane < LANES - 2, right[j], other)
        yield fours + moved(far, j, -2, lane)


def partials_rows(energy, cell, store, count, lane, sub):
    both = ([], [])
    for j in range(count):
        shared = (energy(1, j) + energy(2, j)) + (energy(3, j) + energy(4, j))
        both[0].append(shared + energy(0, j))
        both[1].append(shared + energy(5, j))
    for row, cols in enumerate(both):
        tops, totals, blends = None, [], []
        for j, box in enumerate(box_of(cols, lane)):
            score = box * (sharpness * log2e)
            top = jnp.max(score, axis=0, keepdims=True)
            weight = jnp.exp2(score - top)
            blend = weight * cell(row, j)
            totals.append(weight[0:8] + weight[8:16])
            blends.append(blend[0:8] + blend[8:16])
            tall = jnp.broadcast_to(top, (8, LANES))
            tops = tall if tops is None else jnp.where(sub == j % 8, tall, tops)
            if j % 8 == 7:
                total = gather_sum(totals, sub)
                store(0, row, j - 7, tops + jnp.log2(total))
                store(1, row, j - 7, gather_sum(blends, sub) / total)
                tops, totals, blends = None, [], []


def grid_of(rows, cols):
    return lax.broadcasted_iota(jnp.int32, (rows, cols), 0), lax.broadcasted_iota(jnp.int32, (rows, cols), 1)


def lanes_and_subs(planes):
    return (
        lax.broadcasted_iota(jnp.int32, (planes, LANES), 1),
        lax.broadcasted_iota(jnp.int32, (8, LANES), 0),
    )


def turn_kernel(x_ref, xt_ref, a_ref, b_ref, *, chunk):
    planes, rows, cols = x_ref.shape
    n = planes * rows
    o, k = grid_of(n, n)
    swap = jnp.where((o // planes == k % rows) & (o % planes == k // rows), 1.0, 0.0).astype(jnp.bfloat16)
    for c in range(cols // chunk):
        ds = pl.ds(c * chunk, chunk)
        y = jnp.dot(swap, x_ref[:, :, ds].reshape(n, chunk), preferred_element_type=jnp.float32)
        xt_ref[:, :, ds] = y.reshape(rows, planes, chunk)
    odd = lax.rem(lax.axis_index("xy"), 2)
    last = rows - HALO
    a_ref[...] = xt_ref[pl.ds(last - odd * last, HALO)].astype(jnp.bfloat16)
    b_ref[...] = xt_ref[pl.ds(odd * last, HALO)].astype(jnp.bfloat16)


def inner_kernel(xt_ref, energy_ref, part_ref):
    rows, planes, cols = xt_ref.shape
    count = cols // LANES
    lane, sub = lanes_and_subs(planes)

    def first(r, carry):
        for j, value in energy_row(lambda k, j: xt_ref[r + k, :, tile(j)], count, lane):
            energy_ref[r, :, tile(j)] = value
        return carry

    lax.fori_loop(0, rows - 4, first, 0, unroll=UNROLL)

    def second(h, carry):
        r = 2 * h

        def store(q, row, block, value):
            part_ref[q, r + row, block:block + 8, :] = value

        partials_rows(
            lambda k, j: energy_ref[r + k, :, tile(j)],
            lambda row, j: xt_ref[r + row + 4, :, tile(j)],
            store, count, lane, sub,
        )
        return carry

    lax.fori_loop(0, (rows - 8) // 2, second, 0, unroll=UNROLL2)


def side_rows(below, xt_ref, got_ref, energy_ref, part, cells, energy):
    rows, planes, cols = xt_ref.shape
    count = cols // LANES
    lane, sub = lanes_and_subs(planes)
    me = lax.axis_index("xy")
    at_end = me == jnp.where(below == 1, lax.axis_size("xy") - 1, 0)
    flip = 3 * below
    for i in range(HALO):
        cells[i] = got_ref[i ^ flip].astype(jnp.float32)
        cells[HALO + i] = xt_ref[(rows - HALO) * below + (i ^ flip)]
        energy[HALO + i] = energy_ref[(rows - 8) * below + (i ^ flip)]

    def first(i, carry):
        keep = jnp.where((i < 2) & at_end, 0.0, 1.0)
        for j, value in energy_row(lambda k, j: cells[i + k, :, tile(j)], count, lane):
            energy[i, :, tile(j)] = value * keep
        return carry

    lax.fori_loop(0, HALO, first, 0, unroll=UNROLL)

    def second(h, carry):
        i = 2 * h

        def store(q, row, block, value):
            part[q, HALO * below + ((i + row) ^ flip), block:block + 8, :] = value

        partials_rows(
            lambda k, j: energy[i + k, :, tile(j)],
            lambda row, j: cells[HALO + i + row, :, tile(j)],
            store, count, lane, sub,
        )
        return carry

    lax.fori_loop(0, HALO // 2, second, 0, unroll=UNROLL2)


def near_kernel(xt_ref, got_ref, energy_ref, part_ref, cells, energy):
    below = 1 - lax.rem(lax.axis_index("xy"), 2)
    side_rows(below, xt_ref, got_ref, energy_ref, part_ref, cells, energy)


def far_kernel(xt_ref, got_ref, energy_ref, inner_ref, near_ref, out_ref, cells, energy, part):
    rows, _, cols = xt_ref.shape
    count = cols // LANES
    below = lax.rem(lax.axis_index("xy"), 2)
    side_rows(below, xt_ref, got_ref, energy_ref, part, cells, energy)
    for q in range(2):
        for i in range(HALO):
            slot = HALO * (1 - below) + i
            part[q, slot] = near_ref[q, slot]
    inner_groups, outer_groups = out_ref.shape[:2]
    each = count // (inner_groups * outer_groups)
    for q in range(2):
        for h, ref in enumerate((inner_ref, part)):
            for j in range(count):
                flat = ref.at[q].reshape(8 * count, LANES)
                owner = j // each
                out_ref[owner % inner_groups, owner // inner_groups, q * rows + 8 * h:q * rows + 8 * h + 8,
                        tile(j % each)] = flat[pl.ds(j, 8, stride=count), :]


def merged(entries):
    top = functools.reduce(jnp.maximum, [v for v, _ in entries])
    weights = [jnp.exp2(v - top) for v, _ in entries]
    total = functools.reduce(jnp.add, weights)
    blend = functools.reduce(jnp.add, [w * mean for w, (_, mean) in zip(weights, entries)])
    return top, total, blend / total


def merge_kernel(in_ref, out_ref, *, other):
    inner_groups, _, twice, _ = in_ref.shape
    rows = twice // 2
    mine = lax.axis_index("gz") // inner_groups
    block = 1 - mine if other else mine
    top, total, mean = merged([(in_ref[g, block, 0:rows, :], in_ref[g, block, rows:, :]) for g in range(inner_groups)])
    out_ref[0:rows, :] = top + jnp.log2(total)
    out_ref[rows:, :] = mean


def join_kernel(kept_ref, got_ref, joined_ref, pooled_ref, half):
    twice, own = kept_ref.shape
    rows = twice // 2
    _, _, joined = merged([(ref[0:rows, :], ref[rows:, :]) for ref in (kept_ref, got_ref)])
    joined_ref[HALO:HALO + 8, :] = joined[0:8]
    joined_ref[0:HALO, :] = joined[8:12]
    joined_ref[HALO + 8:rows, :] = joined[12:16]
    halves = []
    for h in range(own // LANES):
        half[h] = joined_ref[:, tile(h)]
        even, uneven = (half.at[h][pl.ds(k, rows // 2, stride=2), :] for k in range(2))
        halves.append(even + uneven)
    halves = jnp.concatenate(halves, axis=1)
    r, c = grid_of(own, own // 2)
    col_pairs = jnp.where(r // 2 == c, 0.25, 0.0)
    pooled_ref[...] = jnp.dot(
        halves, col_pairs, preferred_element_type=jnp.float32, precision=lax.Precision.HIGHEST
    )


def vmem(count):
    return [pl.BlockSpec(memory_space=pltpu.VMEM)] * count


def params(mib):
    return pltpu.CompilerParams(vmem_limit_bytes=mib << 20)


def cost(flops):
    return pl.CostEstimate(flops=flops, bytes_accessed=4 << 20, transcendentals=10**6)


def shards(stack):
    planes, rows, cols = stack.shape
    f32, bf16 = jnp.float32, jnp.bfloat16
    sds = jax.ShapeDtypeStruct
    strip = sds((HALO, planes, cols), bf16)
    count = cols // LANES
    xt, to_a, to_b = pl.pallas_call(
        functools.partial(turn_kernel, chunk=512),
        out_shape=(sds((rows, planes, cols), f32), strip, strip),
        in_specs=vmem(1),
        out_specs=tuple(vmem(3)),
        compiler_params=params(8),
        cost_estimate=cost(10**7),
        name="turn",
    )(stack)
    devices = lax.axis_size("xy")
    ends = [(i, i + 1) for i in range(1, devices - 1, 2)]
    from_b = lax.ppermute(to_b, "xy", ends + [(j, i) for i, j in ends])
    from_a = lax.ppermute(to_a, "xy", [(i, i ^ 1) for i in range(devices)])
    energy, inner = pl.pallas_call(
        inner_kernel,
        out_shape=(sds((rows - 4, planes, cols), f32), sds((2, rows - 8, count, LANES), f32)),
        in_specs=vmem(1),
        out_specs=tuple(vmem(2)),
        compiler_params=params(8),
        cost_estimate=cost(10**8),
        name="inner",
    )(xt)
    side_scratch = [pltpu.VMEM((2 * HALO, planes, cols), f32)] * 2
    part = sds((2, 2 * HALO, count, LANES), f32)
    near = pl.pallas_call(
        near_kernel,
        out_shape=part,
        in_specs=vmem(3),
        out_specs=vmem(1)[0],
        scratch_shapes=side_scratch,
        compiler_params=params(8),
        cost_estimate=cost(10**8),
        name="near",
    )(xt, from_a, energy)
    groups = lax.axis_size("gz")
    own = cols // groups
    outer_groups = 2
    inner_groups = groups // outer_groups
    ready = pl.pallas_call(
        far_kernel,
        out_shape=sds((inner_groups, outer_groups, 2 * rows, own), f32),
        in_specs=vmem(5),
        out_specs=vmem(1)[0],
        scratch_shapes=side_scratch + [pltpu.VMEM(part.shape, f32)],
        compiler_params=params(8),
        cost_estimate=cost(10**8),
        name="far",
    )(xt, from_b, energy, inner, near)
    teams = [[o * inner_groups + i for i in range(inner_groups)] for o in range(outer_groups)]
    parts = lax.all_to_all(ready, "gz", split_axis=0, concat_axis=0, tiled=True, axis_index_groups=teams)

    def merge(other):
        return pl.pallas_call(
            functools.partial(merge_kernel, other=other),
            out_shape=sds((2 * rows, own), f32),
            in_specs=vmem(1),
            out_specs=vmem(1)[0],
            compiler_params=params(4),
            cost_estimate=cost(10**6),
            name="merge_other" if other else "merge_own",
        )(parts)

    leaving = merge(True)
    got = lax.ppermute(leaving, "gz", [(i, (i + inner_groups) % groups) for i in range(groups)])
    kept = merge(False)
    return pl.pallas_call(
        join_kernel,
        out_shape=(sds((rows, own), f32), sds((rows // 2, own // 2), f32)),
        in_specs=vmem(2),
        out_specs=tuple(vmem(2)),
        scratch_shapes=[pltpu.VMEM((own // LANES, rows, LANES), f32)],
        compiler_params=params(4),
        name="join",
    )(kept, got)


def solution(mesh):
    in_specs = (P("gz", "xy", None),)
    out_specs = (P("xy", "gz"), P("xy", "gz"))
    return jax.shard_map(shards, mesh=mesh, in_specs=in_specs, out_specs=out_specs, check_vma=False)
```

```python
import functools

import jax
import jax.numpy as jnp
from jax import lax
from jax.experimental import pallas as pl
from jax.experimental.pallas import tpu as pltpu
from jax.sharding import PartitionSpec as P


sharpness = 0.016
log2e = 1.4426950408889634
LANES = 128
HALO = 4
UNROLL = 4
UNROLL2 = 1
AHEAD1 = 8
AHEAD2 = 4


def tile(j):
    return pl.ds(j * LANES, LANES)


def moved(turned, j, step, lane):
    if step > 0:
        other = turned[j + 1] if j + 1 < len(turned) else jnp.zeros_like(turned[j])
        return jnp.where(lane < LANES - step, turned[j], other)
    other = turned[j - 1] if j > 0 else jnp.zeros_like(turned[j])
    return jnp.where(lane >= -step, turned[j], other)


def rotated(tiles, step):
    return [pltpu.roll(t, (-step) % LANES, axis=1) for t in tiles]


def energy_row(load, count, lane):
    turned = {step: [] for step in (1, -1, 2, -2)}
    middles = []

    def begin(j):
        cell = load(2, j)
        beside = (cell + cell) + (load(1, j) + load(3, j))
        half = cell.astype(jnp.bfloat16)
        for step in (1, -1):
            turned[step] += rotated([beside], step)
        for step in (2, -2):
            turned[step] += [t.astype(jnp.float32) for t in rotated([half], step)]
        middles.append((20.0 * cell - (beside + beside)) - (load(0, j) + load(4, j)))

    def shifted(j, step):
        tiles = turned[step]
        k = j + (1 if step > 0 else -1)
        other = tiles[k] if 0 <= k < count else jnp.zeros_like(tiles[j])
        return jnp.where(lane < LANES - step if step > 0 else lane >= -step, tiles[j], other)

    ahead = 8
    for j in range(min(ahead, count)):
        begin(j)
    for j in range(count):
        if j + ahead < count:
            begin(j + ahead)
        lap = middles[j] - (shifted(j, 1) + shifted(j, -1)) - (shifted(j, 2) + shifted(j, -2))
        yield j, lap * lap


def gather_sum(tiles, sub):
    low = sub < 4
    tiles = [
        jnp.where(low, a, b) + pltpu.roll(jnp.where(low, b, a), 4, axis=0) for a, b in zip(tiles[:4], tiles[4:])
    ]
    for d in (2, 1):
        pick = (sub & d) == 0
        tiles = [
            jnp.where(pick, a + pltpu.roll(a, 8 - d, axis=0), b + pltpu.roll(b, d, axis=0))
            for a, b in zip(tiles[:d], tiles[d:])
        ]
    return tiles[0]


def box_steps(col, count, lane):
    cols, left, far, pairs, right = [], [], [], [], []

    def first():
        c = col(len(cols))
        cols.append(c)
        left.extend(rotated([c], -1))
        far.extend(rotated([c], -2))

    def second():
        j = len(pairs)
        pairs.append(cols[j] + moved(left, j, -1, lane))
        right.extend(rotated(pairs[-1:], 2))

    for j in range(count):
        while len(cols) < min(j + AHEAD1, count):
            first()
        while len(pairs) < min(j + AHEAD2, count):
            second()
        if j + 1 < count:
            other = right[j + 1]
        else:
            other = jnp.where(lane == LANES - 2, pltpu.roll(cols[-1], LANES - 1, axis=1), 0.0)
        yield pairs[j] + jnp.where(lane < LANES - 2, right[j], other) + moved(far, j, -2, lane)


def partials_rows(energy, cell, store, count, lane, sub):
    shared = {}

    def col(row, j):
        if j not in shared:
            shared[j] = (energy(1, j) + energy(2, j)) + (energy(3, j) + energy(4, j))
        return shared[j] + energy(5 * row, j)

    steps = [box_steps(functools.partial(col, row), count, lane) for row in range(2)]
    state = [[None, [], []] for _ in range(2)]
    for j in range(count):
        for row in range(2):
            score = next(steps[row]) * (sharpness * log2e)
            tops, totals, blends = state[row]
            top = jnp.max(score, axis=0, keepdims=True)
            weight = jnp.exp2(score - top)
            blend = weight * cell(row, j)
            totals.append(weight[0:8] + weight[8:16])
            blends.append(blend[0:8] + blend[8:16])
            tall = jnp.broadcast_to(top, (8, LANES))
            state[row][0] = tall if tops is None else jnp.where(sub == j % 8, tall, tops)
            if j % 8 == 7:
                total = gather_sum(totals, sub)
                store(0, row, j - 7, state[row][0] + jnp.log2(total))
                store(1, row, j - 7, gather_sum(blends, sub) / total)
                state[row] = [None, [], []]


def grid_of(rows, cols):
    return lax.broadcasted_iota(jnp.int32, (rows, cols), 0), lax.broadcasted_iota(jnp.int32, (rows, cols), 1)


def lanes_and_subs(planes):
    return (
        lax.broadcasted_iota(jnp.int32, (planes, LANES), 1),
        lax.broadcasted_iota(jnp.int32, (8, LANES), 0),
    )


def turn_kernel(x_ref, xt_ref, a_ref, b_ref, *, chunk):
    planes, rows, cols = x_ref.shape
    n = planes * rows
    o, k = grid_of(n, n)
    swap = jnp.where((o // planes == k % rows) & (o % planes == k // rows), 1.0, 0.0).astype(jnp.bfloat16)
    for c in range(cols // chunk):
        ds = pl.ds(c * chunk, chunk)
        y = jnp.dot(swap, x_ref[:, :, ds].reshape(n, chunk), preferred_element_type=jnp.float32)
        xt_ref[:, :, ds] = y.reshape(rows, planes, chunk)
    odd = lax.rem(lax.axis_index("xy"), 2)
    last = rows - HALO
    a_ref[...] = xt_ref[pl.ds(last - odd * last, HALO)].astype(jnp.bfloat16)
    b_ref[...] = xt_ref[pl.ds(odd * last, HALO)].astype(jnp.bfloat16)


def inner_kernel(xt_ref, energy_ref, part_ref):
    rows, planes, cols = xt_ref.shape
    count = cols // LANES
    lane, sub = lanes_and_subs(planes)

    def first(r, carry):
        for j, value in energy_row(lambda k, j: xt_ref[r + k, :, tile(j)], count, lane):
            energy_ref[r, :, tile(j)] = value
        return carry

    lax.fori_loop(0, rows - 4, first, 0, unroll=UNROLL)

    def second(h, carry):
        r = 2 * h

        def store(q, row, block, value):
            part_ref[q, r + row, block:block + 8, :] = value

        partials_rows(
            lambda k, j: energy_ref[r + k, :, tile(j)],
            lambda row, j: xt_ref[r + row + 4, :, tile(j)],
            store, count, lane, sub,
        )
        return carry

    lax.fori_loop(0, (rows - 8) // 2, second, 0, unroll=UNROLL2)


def side_rows(below, xt_ref, got_ref, energy_ref, part, cells, energy):
    rows, planes, cols = xt_ref.shape
    count = cols // LANES
    lane, sub = lanes_and_subs(planes)
    me = lax.axis_index("xy")
    at_end = me == jnp.where(below == 1, lax.axis_size("xy") - 1, 0)
    flip = 3 * below
    for i in range(HALO):
        cells[i] = got_ref[i ^ flip].astype(jnp.float32)
        cells[HALO + i] = xt_ref[(rows - HALO) * below + (i ^ flip)]
        energy[HALO + i] = energy_ref[(rows - 8) * below + (i ^ flip)]

    def first(i, carry):
        keep = jnp.where((i < 2) & at_end, 0.0, 1.0)
        for j, value in energy_row(lambda k, j: cells[i + k, :, tile(j)], count, lane):
            energy[i, :, tile(j)] = value * keep
        return carry

    lax.fori_loop(0, HALO, first, 0, unroll=UNROLL)

    def second(h, carry):
        i = 2 * h

        def store(q, row, block, value):
            part[q, HALO * below + ((i + row) ^ flip), block:block + 8, :] = value

        partials_rows(
            lambda k, j: energy[i + k, :, tile(j)],
            lambda row, j: cells[HALO + i + row, :, tile(j)],
            store, count, lane, sub,
        )
        return carry

    lax.fori_loop(0, HALO // 2, second, 0, unroll=UNROLL2)


def near_kernel(xt_ref, got_ref, energy_ref, part_ref, cells, energy):
    below = 1 - lax.rem(lax.axis_index("xy"), 2)
    side_rows(below, xt_ref, got_ref, energy_ref, part_ref, cells, energy)


def far_kernel(xt_ref, got_ref, energy_ref, inner_ref, near_ref, out_ref, cells, energy, part):
    rows, _, cols = xt_ref.shape
    count = cols // LANES
    below = lax.rem(lax.axis_index("xy"), 2)
    side_rows(below, xt_ref, got_ref, energy_ref, part, cells, energy)
    for q in range(2):
        for i in range(HALO):
            slot = HALO * (1 - below) + i
            part[q, slot] = near_ref[q, slot]
    inner_groups, outer_groups = out_ref.shape[:2]
    each = count // (inner_groups * outer_groups)
    for q in range(2):
        for h, ref in enumerate((inner_ref, part)):
            for j in range(count):
                flat = ref.at[q].reshape(8 * count, LANES)
                owner = j // each
                out_ref[owner % inner_groups, owner // inner_groups, q * rows + 8 * h:q * rows + 8 * h + 8,
                        tile(j % each)] = flat[pl.ds(j, 8, stride=count), :]


def merged(entries):
    top = functools.reduce(jnp.maximum, [v for v, _ in entries])
    weights = [jnp.exp2(v - top) for v, _ in entries]
    total = functools.reduce(jnp.add, weights)
    blend = functools.reduce(jnp.add, [w * mean for w, (_, mean) in zip(weights, entries)])
    return top, total, blend / total


def merge_kernel(in_ref, out_ref, *, other):
    inner_groups, _, twice, _ = in_ref.shape
    rows = twice // 2
    mine = lax.axis_index("gz") // inner_groups
    block = 1 - mine if other else mine
    top, total, mean = merged([(in_ref[g, block, 0:rows, :], in_ref[g, block, rows:, :]) for g in range(inner_groups)])
    out_ref[0:rows, :] = top + jnp.log2(total)
    out_ref[rows:, :] = mean


def join_kernel(kept_ref, got_ref, joined_ref, pooled_ref, half):
    twice, own = kept_ref.shape
    rows = twice // 2
    _, _, joined = merged([(ref[0:rows, :], ref[rows:, :]) for ref in (kept_ref, got_ref)])
    joined_ref[HALO:HALO + 8, :] = joined[0:8]
    joined_ref[0:HALO, :] = joined[8:12]
    joined_ref[HALO + 8:rows, :] = joined[12:16]
    halves = []
    for h in range(own // LANES):
        half[h] = joined_ref[:, tile(h)]
        even, uneven = (half.at[h][pl.ds(k, rows // 2, stride=2), :] for k in range(2))
        halves.append(even + uneven)
    halves = jnp.concatenate(halves, axis=1)
    r, c = grid_of(own, own // 2)
    col_pairs = jnp.where(r // 2 == c, 0.25, 0.0)
    pooled_ref[...] = jnp.dot(
        halves, col_pairs, preferred_element_type=jnp.float32, precision=lax.Precision.HIGHEST
    )


def vmem(count):
    return [pl.BlockSpec(memory_space=pltpu.VMEM)] * count


def params(mib):
    return pltpu.CompilerParams(vmem_limit_bytes=mib << 20)


def cost(flops):
    return pl.CostEstimate(flops=flops, bytes_accessed=4 << 20, transcendentals=10**6)


def shards(stack):
    planes, rows, cols = stack.shape
    f32, bf16 = jnp.float32, jnp.bfloat16
    sds = jax.ShapeDtypeStruct
    strip = sds((HALO, planes, cols), bf16)
    count = cols // LANES
    xt, to_a, to_b = pl.pallas_call(
        functools.partial(turn_kernel, chunk=512),
        out_shape=(sds((rows, planes, cols), f32), strip, strip),
        in_specs=vmem(1),
        out_specs=tuple(vmem(3)),
        compiler_params=params(8),
        cost_estimate=cost(10**7),
        name="turn",
    )(stack)
    devices = lax.axis_size("xy")
    ends = [(i, i + 1) for i in range(1, devices - 1, 2)]
    from_b = lax.ppermute(to_b, "xy", ends + [(j, i) for i, j in ends])
    from_a = lax.ppermute(to_a, "xy", [(i, i ^ 1) for i in range(devices)])
    energy, inner = pl.pallas_call(
        inner_kernel,
        out_shape=(sds((rows - 4, planes, cols), f32), sds((2, rows - 8, count, LANES), f32)),
        in_specs=vmem(1),
        out_specs=tuple(vmem(2)),
        compiler_params=params(8),
        cost_estimate=cost(10**8),
        name="inner",
    )(xt)
    side_scratch = [pltpu.VMEM((2 * HALO, planes, cols), f32)] * 2
    part = sds((2, 2 * HALO, count, LANES), f32)
    near = pl.pallas_call(
        near_kernel,
        out_shape=part,
        in_specs=vmem(3),
        out_specs=vmem(1)[0],
        scratch_shapes=side_scratch,
        compiler_params=params(8),
        cost_estimate=cost(10**8),
        name="near",
    )(xt, from_a, energy)
    groups = lax.axis_size("gz")
    own = cols // groups
    outer_groups = 2
    inner_groups = groups // outer_groups
    ready = pl.pallas_call(
        far_kernel,
        out_shape=sds((inner_groups, outer_groups, 2 * rows, own), f32),
        in_specs=vmem(5),
        out_specs=vmem(1)[0],
        scratch_shapes=side_scratch + [pltpu.VMEM(part.shape, f32)],
        compiler_params=params(8),
        cost_estimate=cost(10**8),
        name="far",
    )(xt, from_b, energy, inner, near)
    teams = [[o * inner_groups + i for i in range(inner_groups)] for o in range(outer_groups)]
    parts = lax.all_to_all(ready, "gz", split_axis=0, concat_axis=0, tiled=True, axis_index_groups=teams)

    def merge(other):
        return pl.pallas_call(
            functools.partial(merge_kernel, other=other),
            out_shape=sds((2 * rows, own), f32),
            in_specs=vmem(1),
            out_specs=vmem(1)[0],
            compiler_params=params(4),
            cost_estimate=cost(10**6),
            name="merge_other" if other else "merge_own",
        )(parts)

    leaving = merge(True)
    got = lax.ppermute(leaving, "gz", [(i, (i + inner_groups) % groups) for i in range(groups)])
    kept = merge(False)
    return pl.pallas_call(
        join_kernel,
        out_shape=(sds((rows, own), f32), sds((rows // 2, own // 2), f32)),
        in_specs=vmem(2),
        out_specs=tuple(vmem(2)),
        scratch_shapes=[pltpu.VMEM((own // LANES, rows, LANES), f32)],
        compiler_params=params(4),
        name="join",
    )(kept, got)


def solution(mesh):
    in_specs = (P("gz", "xy", None),)
    out_specs = (P("xy", "gz"), P("xy", "gz"))
    return jax.shard_map(shards, mesh=mesh, in_specs=in_specs, out_specs=out_specs, check_vma=False)
```
